32 devices in a mesh: dp: 4 (over y, core), wide: 8 (over z, x).
Axes of the slice: x: 2, y: 2, z: 4, core: 2. Of those that a mesh axis runs over, the one named last changes fastest.
Arguments:
- fields: bfloat16 [16, 64, 128, 1280], P('dp', 'wide'), may hold values from -6 to 6
- targets: bfloat16 [16, 64, 128, 1280], P('dp', 'wide'), may hold values from -6 to 6
- patch_mask: int32 [16, 64, 128], P('dp', 'wide'), may hold values from 0 to 1, as said below
- channel_mask: int32 [16, 20], P('dp'), may hold values from 0 to 1, as said below
- embed_weight: float32 [1280, 768], P(('dp', 'wide')), may hold values from -0.15625 to 0.15625
- head_weight: float32 [768, 1280], P(('dp', 'wide')), may hold values from -0.21875 to 0.21875
- expand_weight: float32 [768, 3072], P(('dp', 'wide')), may hold values from -0.21875 to 0.21875
- project_weight: float32 [3072, 768], P(('dp', 'wide')), may hold values from -0.109375 to 0.109375
- spectral_weight: float32 [2, 2, 768, 96], P(None, None, ('dp', 'wide')), may hold values from -0.4375 to 0.4375
- small_params: float32 [14, 768], P(None, ('dp', 'wide')), may hold values from -1.2 to 1.3
- embed_moment: float32 [1280, 768], P(('dp', 'wide'))
- head_moment: float32 [768, 1280], P(('dp', 'wide'))
- expand_moment: float32 [768, 3072], P(('dp', 'wide'))
- project_moment: float32 [3072, 768], P(('dp', 'wide'))
- spectral_moment: float32 [2, 2, 768, 96], P(None, None, ('dp', 'wide'))
- small_moment: float32 [14, 768], P(None, ('dp', 'wide'))
- embed_square: float32 [1280, 768], P(('dp', 'wide'))
- head_square: float32 [768, 1280], P(('dp', 'wide'))
- expand_square: float32 [768, 3072], P(('dp', 'wide'))
- project_square: float32 [3072, 768], P(('dp', 'wide'))
- spectral_square: float32 [2, 2, 768, 96], P(None, None, ('dp', 'wide'))
- small_square: float32 [14, 768], P(None, ('dp', 'wide'))
Outputs:
- loss: float32 [], replicated
- grad_norm: float32 [], replicated
- embed_next: float32 [1280, 768], P(('dp', 'wide'))
- embed_moment_next: float32 [1280, 768], P(('dp', 'wide'))
- embed_square_next: float32 [1280, 768], P(('dp', 'wide'))
- head_next: float32 [768, 1280], P(('dp', 'wide'))
- head_moment_next: float32 [768, 1280], P(('dp', 'wide'))
- head_square_next: float32 [768, 1280], P(('dp', 'wide'))
- expand_next: float32 [768, 3072], P(('dp', 'wide'))
- expand_moment_next: float32 [768, 3072], P(('dp', 'wide'))
- expand_square_next: float32 [768, 3072], P(('dp', 'wide'))
- project_next: float32 [3072, 768], P(('dp', 'wide'))
- project_moment_next: float32 [3072, 768], P(('dp', 'wide'))
- project_square_next: float32 [3072, 768], P(('dp', 'wide'))
- spectral_next: float32 [2, 2, 768, 96], P(None, None, ('dp', 'wide'))
- spectral_moment_next: float32 [2, 2, 768, 96], P(None, None, ('dp', 'wide'))
- spectral_square_next: float32 [2, 2, 768, 96], P(None, None, ('dp', 'wide'))
- small_next: float32 [14, 768], P(None, ('dp', 'wide'))
- small_moment_next: float32 [14, 768], P(None, ('dp', 'wide'))
- small_square_next: float32 [14, 768], P(None, ('dp', 'wide'))
The draws below stay inside these ranges and needn't reach their ends.
Inputs may be any that keep to these rules, and one draw needn't show every extreme that they name: `patch_mask`: A sample of the coarse group other than the first has valid patches only in its first 32 rows and 64 columns; the first grid row of the first sample is all valid. `channel_mask`: the first sample observes every channel.
All inputs are finite; a program needn't handle non-finite values.
Results may differ from the reference program's by a relative error of at most 0.0055.
The reference program's roundings to bfloat16 on the way count: a program that leaves them out, or rounds other values in their place, can miss the bound.
Values may be sent and summed in bfloat16 or wider, within the bound.
A program may use at most 512 MiB of HBM per device.

```python
import jax
import jax.numpy as jnp
from jax import lax

D = 768
NB = 8
BS = 96
FF = 3072
PATCH = 8
CH = 20
PD = 1280
H = 64
W = 128
KW = 64
BATCH = 16


def grad_scale(boost):
    params_all = 2 * PD * D + 2 * D * FF + 4 * D * BS + 14 * D
    clip_level = 0.25 / jnp.sqrt(jnp.float32(BATCH * H * W))
    return boost * 2.0 * clip_level / jnp.sqrt(jnp.float32(params_all))


def first_moment(key, tag, shape, boost):
    noise = jnp.clip(jax.random.normal(jax.random.fold_in(key, tag), shape, jnp.float32), -4.0, 4.0)
    return 0.11 * grad_scale(boost) * noise


def second_moment(key, tag, shape, boost):
    level = jax.random.uniform(jax.random.fold_in(key, tag), shape, jnp.float32, jnp.log(0.053), jnp.log(0.21))
    return jnp.exp(level) * grad_scale(boost) ** 2


def draw_patch_mask(key, part):
    group = jax.random.randint(jax.random.fold_in(key, 1), (BATCH, 1, 1), 0, 2)
    rows = jnp.arange(H, dtype=jnp.int32)[None, :, None]
    cols = jnp.arange(W, dtype=jnp.int32)[None, None, :]
    inside = (group == 0) | (rows < H // 2) & (cols < W // 2)
    keep = jax.random.randint(jax.random.fold_in(key, 2), (BATCH, H, W), 0, 10) > 0
    first = (jnp.arange(BATCH, dtype=jnp.int32)[:, None, None] == 0) & (rows == 0)
    return (inside & keep | first).astype(jnp.int32)


def draw_channel_mask(key, part):
    keep = jax.random.randint(jax.random.fold_in(key, 3), (BATCH, CH), 0, 5) > 0
    first = jnp.arange(BATCH, dtype=jnp.int32)[:, None] == 0
    return (keep | first).astype(jnp.int32)


def draw_small_params(key, part):
    noise = jax.random.normal(jax.random.fold_in(key, 4), (14, D), jnp.float32)
    rows = jnp.arange(14, dtype=jnp.int32)[:, None]
    gain_rows = (rows == 0) | (rows == 2)
    return jnp.where(gain_rows, 1.0 + 0.1 * jnp.clip(noise, -3.0, 3.0), 0.3 * jnp.clip(noise, -4.0, 4.0))


def draw_embed_moment(key, part):
    return first_moment(key, 11, (PD, D), 1.0)


def draw_head_moment(key, part):
    return first_moment(key, 12, (D, PD), 1.0)


def draw_expand_moment(key, part):
    return first_moment(key, 13, (D, FF), 1.0)


def draw_project_moment(key, part):
    return first_moment(key, 14, (FF, D), 1.0)


def draw_spectral_moment(key, part):
    return first_moment(key, 15, (2, 2, D, BS), 2.0)


def draw_small_moment(key, part):
    return first_moment(key, 16, (14, D), 10.0)


def draw_embed_square(key, part):
    return second_moment(key, 21, (PD, D), 1.0)


def draw_head_square(key, part):
    return second_moment(key, 22, (D, PD), 1.0)


def draw_expand_square(key, part):
    return second_moment(key, 23, (D, FF), 1.0)


def draw_project_square(key, part):
    return second_moment(key, 24, (FF, D), 1.0)


def draw_spectral_square(key, part):
    return second_moment(key, 25, (2, 2, D, BS), 2.0)


def draw_small_square(key, part):
    return second_moment(key, 26, (14, D), 10.0)


def block_levels(key, dims, split, smallest, high):
    level = 1.0
    for dim, shards_of in split:
        draws = jax.random.uniform(jax.random.fold_in(jax.random.fold_in(key, 6), dim), (shards_of,), jnp.float32, smallest / len(split), high / len(split))
        level = level * jnp.repeat(jnp.exp(draws), dims[dim] // shards_of).reshape((-1,) + (1,) * (len(dims) - 1 - dim))
    return level


def normal_values(key, dims, deviation, most, split=(), kind=jnp.bfloat16):
    loudness = block_levels(key, dims, split, -0.22, 0.18) if split else 1.0
    drawn = jax.random.normal(key, dims, jnp.float32) * deviation * loudness
    return jnp.minimum(jnp.maximum(drawn, -most), most).astype(kind)


def setup_inputs(seed: int = 0) -> dict:
    seeds = jax.random.split(jax.random.key(seed), 23)
    fields = normal_values(seeds[0], (BATCH, H, W, PD), 1.0, 6.0, ((0, 4), (1, 8)))
    targets = normal_values(seeds[1], (BATCH, H, W, PD), 1.0, 6.0, ((0, 4), (1, 8)))
    patch_mask = draw_patch_mask(jax.random.fold_in(seeds[22], 71), 0)
    channel_mask = draw_channel_mask(jax.random.fold_in(seeds[22], 71), 0)
    embed_weight = normal_values(seeds[4], (PD, D), PD ** -0.5, 0.15625, ((0, 32),), jnp.float32)
    head_weight = normal_values(seeds[5], (D, PD), D ** -0.5, 0.21875, ((0, 32),), jnp.float32)
    expand_weight = normal_values(seeds[6], (D, FF), D ** -0.5, 0.21875, ((0, 32),), jnp.float32)
    project_weight = normal_values(seeds[7], (FF, D), FF ** -0.5, 0.109375, ((0, 32),), jnp.float32)
    spectral_weight = normal_values(seeds[8], (2, 2, D, BS), (2 * BS) ** -0.5, 0.4375, ((2, 32),), jnp.float32)
    small_params = draw_small_params(jax.random.fold_in(seeds[22], 71), 0)
    embed_moment = draw_embed_moment(jax.random.fold_in(seeds[22], 71), 0)
    head_moment = draw_head_moment(jax.random.fold_in(seeds[22], 71), 0)
    expand_moment = draw_expand_moment(jax.random.fold_in(seeds[22], 71), 0)
    project_moment = draw_project_moment(jax.random.fold_in(seeds[22], 71), 0)
    spectral_moment = draw_spectral_moment(jax.random.fold_in(seeds[22], 71), 0)
    small_moment = draw_small_moment(jax.random.fold_in(seeds[22], 71), 0)
    embed_square = draw_embed_square(jax.random.fold_in(seeds[22], 71), 0)
    head_square = draw_head_square(jax.random.fold_in(seeds[22], 71), 0)
    expand_square = draw_expand_square(jax.random.fold_in(seeds[22], 71), 0)
    project_square = draw_project_square(jax.random.fold_in(seeds[22], 71), 0)
    spectral_square = draw_spectral_square(jax.random.fold_in(seeds[22], 71), 0)
    small_square = draw_small_square(jax.random.fold_in(seeds[22], 71), 0)
    return dict(fields=fields, targets=targets, patch_mask=patch_mask, channel_mask=channel_mask, embed_weight=embed_weight, head_weight=head_weight, expand_weight=expand_weight, project_weight=project_weight, spectral_weight=spectral_weight, small_params=small_params, embed_moment=embed_moment, head_moment=head_moment, expand_moment=expand_moment, project_moment=project_moment, spectral_moment=spectral_moment, small_moment=small_moment, embed_square=embed_square, head_square=head_square, expand_square=expand_square, project_square=project_square, spectral_square=spectral_square, small_square=small_square)


EPSILON = 1e-06
SHRINK = 0.01
BETA_ONE = 0.9
BETA_TWO = 0.95
RATES = (0.08, 0.1, 0.1, 0.05, 0.3, 0.5)
DECAYS = (0.1, 0.1, 0.1, 0.1, 0.1, 0.0)
HIGHEST = lax.Precision.HIGHEST

@jax.custom_vjp
def low(v):
    return lax.optimization_barrier(v.astype(jnp.bfloat16)).astype(jnp.float32)

@jax.custom_vjp
def low_back(v):
    return v

def low_keep(v):
    return (low(v), None)

def low_pass(kept, grad):
    return (grad,)

def back_keep(v):
    return (v, None)

def back_low(kept, grad):
    return (low(grad),)
low.defvjp(low_keep, low_pass)
low_back.defvjp(back_keep, back_low)

def layer_norm(values, gain, shift):
    centred = values - lax.optimization_barrier(jnp.mean(values, axis=-1, keepdims=True))
    spread = lax.optimization_barrier(jnp.mean(centred * centred, axis=-1, keepdims=True))
    return centred * lax.rsqrt(spread + EPSILON) * gain + shift

def make_tables():
    across = jnp.arange(W, dtype=jnp.int32)
    freqs = jnp.arange(KW, dtype=jnp.int32)
    angles = 2.0 * jnp.pi / W * (across[:, None] * freqs[None, :] % W).astype(jnp.float32)
    row_table = low(jnp.stack([jnp.cos(angles), -jnp.sin(angles)], axis=1) / jnp.sqrt(jnp.float32(W)))
    doubling = jnp.where(freqs == 0, 1.0, 2.0).astype(jnp.float32)
    inv_table = row_table * doubling
    down = jnp.arange(H, dtype=jnp.int32)
    col_angles = 2.0 * jnp.pi / H * (down[:, None] * down[None, :] % H).astype(jnp.float32)
    cosine = jnp.cos(col_angles) / jnp.sqrt(jnp.float32(H))
    sine = jnp.sin(col_angles) / jnp.sqrt(jnp.float32(H))
    col_table = low(jnp.stack([jnp.stack([cosine, sine]), jnp.stack([-sine, cosine])]))
    return (row_table, inv_table, col_table)

def complex_mix(spec, weight, bias):
    shape = spec.shape
    blocks = spec.reshape(-1, 2, shape[-2], NB, BS)
    kernel = weight.reshape(2, NB, BS, BS)
    prods = jnp.einsum('xakbi,cbij->xackbj', blocks, kernel, precision=HIGHEST)
    real_part = prods[:, 0, 0] - prods[:, 1, 1]
    imag_part = prods[:, 0, 1] + prods[:, 1, 0]
    return jnp.stack([real_part, imag_part], axis=1).reshape(shape) + bias[:, None, :]

def sample_loss(params, tables, sample, scale_cols):
    embed_used, head_used, expand_used, project_used, spectral_used, small_used = params
    row_table, inv_table, col_table = tables
    field, target, pmask, cmask = sample
    valid_patch = pmask.astype(jnp.float32)
    inputs = (field.astype(jnp.float32) * valid_patch[:, :, None]).reshape(H * W, PD)
    hidden_zero = low_back(jnp.dot(inputs, embed_used, precision=HIGHEST) + small_used[4])
    normed_one = layer_norm(hidden_zero, small_used[0], small_used[1])
    normed_low = low(normed_one).reshape(H, W, D)
    rows_freq = low_back(low(jnp.einsum('hwd,wak->hakd', normed_low, row_table, precision=HIGHEST)))
    spectrum = low_back(low(jnp.einsum('oaxi,iakd->xokd', col_table, rows_freq, precision=HIGHEST)))
    first_pre = low_back(complex_mix(spectrum, spectral_used[0], small_used[10:12]))
    first_act = low(jax.nn.relu(first_pre))
    second_pre = low_back(complex_mix(first_act, spectral_used[1], small_used[12:14]))
    shrunk = low(second_pre - jnp.clip(second_pre, -SHRINK, SHRINK))
    back_cols = low_back(low(jnp.einsum('aoxi,xakd->iokd', col_table, shrunk, precision=HIGHEST)))
    filtered = low_back(jnp.einsum('wak,hakd->hwd', inv_table, back_cols, precision=HIGHEST)).reshape(H * W, D)
    hidden_one = hidden_zero + filtered + normed_one
    normed_two = low(layer_norm(hidden_one, small_used[2], small_used[3]))
    expand_pre = low_back(jnp.dot(normed_two, expand_used, precision=HIGHEST) + small_used[6:10].reshape(-1))
    expand_act = low(jax.nn.gelu(expand_pre, approximate=False))
    branch_out = low_back(jnp.dot(expand_act, project_used, precision=HIGHEST) + small_used[5])
    hidden_two = hidden_one + branch_out
    predict = low_back(jnp.dot(low(hidden_two), head_used, precision=HIGHEST))
    errors = predict - target.astype(jnp.float32).reshape(H * W, PD)
    weighted = valid_patch.reshape(H * W, 1) * jnp.repeat(cmask.astype(jnp.float32), PATCH * PATCH)[None, :]
    return jnp.sum(errors * errors * weighted * scale_cols[None, :])

def adam_update(master, moment, square, grad, factor, rate, decay):
    clipped = grad * factor
    moment_next = BETA_ONE * moment + (1.0 - BETA_ONE) * clipped
    square_next = BETA_TWO * square + (1.0 - BETA_TWO) * clipped * clipped
    ratio = moment_next / (1.0 - BETA_ONE ** 10) / (jnp.sqrt(square_next / (1.0 - BETA_TWO ** 10)) + 1e-08)
    return (master - rate * (ratio + decay * master), moment_next, square_next)

def reference(fields, targets, patch_mask, channel_mask, embed_weight, head_weight, expand_weight, project_weight, spectral_weight, small_params, embed_moment, head_moment, expand_moment, project_moment, spectral_moment, small_moment, embed_square, head_square, expand_square, project_square, spectral_square, small_square):
    masters = (embed_weight, head_weight, expand_weight, project_weight, spectral_weight, small_params)
    moments = (embed_moment, head_moment, expand_moment, project_moment, spectral_moment, small_moment)
    squares = (embed_square, head_square, expand_square, project_square, spectral_square, small_square)
    tables = make_tables()
    per_sample = lax.optimization_barrier(jnp.sum(patch_mask.astype(jnp.float32), axis=(1, 2)))
    counts = lax.optimization_barrier(jnp.sum(channel_mask.astype(jnp.float32) * per_sample[:, None], axis=0)) * (PATCH * PATCH)
    scale_cols = jnp.repeat(1.0 / (CH * counts), PATCH * PATCH)

    def total_loss(params):
        rounded = tuple((low(param) for param in params))

        def one_sample(carry, sample):
            return (carry + sample_loss(rounded, tables, sample, scale_cols), None)
        total, _ = lax.scan(jax.checkpoint(one_sample), jnp.zeros((), jnp.float32), (fields, targets, patch_mask, channel_mask))
        return total
    loss, pullback = jax.vjp(total_loss, masters)
    grads = pullback(jnp.ones((), jnp.float32))[0]
    grad_norm = jnp.sqrt(sum((jnp.sum(grad * grad) for grad in grads)))
    clip_level = 0.25 / jnp.sqrt(jnp.float32(BATCH * H * W))
    factor = jnp.minimum(1.0, clip_level / grad_norm)
    results = [loss, grad_norm]
    for index in range(6):
        results.extend(adam_update(masters[index], moments[index], squares[index], grads[index], factor, RATES[index], DECAYS[index]))
    return tuple(results)
```

```python
import jax
import jax.numpy as jnp
from jax import lax
from jax.sharding import PartitionSpec as P

EPSILON = 1e-06
SHRINK = 0.01
BETA_ONE = 0.9
BETA_TWO = 0.95
RATES = (0.08, 0.1, 0.1, 0.05, 0.3, 0.5)
DECAYS = (0.1, 0.1, 0.1, 0.1, 0.1, 0.0)
AXES = ("dp", "wide")
UNUSED = 64.0
BF16 = jnp.bfloat16
F32 = jnp.float32


def dot(left, right, dims):
    return lax.dot_general(left, right, (dims, ((), ())), preferred_element_type=F32)


def normalize(values):
    centred = values - jnp.mean(values, axis=-1, keepdims=True)
    spread = jnp.mean(centred * centred, axis=-1, keepdims=True)
    rstd = lax.rsqrt(spread + EPSILON)
    return centred * rstd, rstd


def norm_back(grad, unit, rstd, gain):
    scaled = grad * gain
    first = jnp.mean(scaled, axis=-1, keepdims=True)
    second = jnp.mean(scaled * unit, axis=-1, keepdims=True)
    back = rstd * (scaled - first - unit * second)
    return back, jnp.sum(grad * unit, axis=0), jnp.sum(grad, axis=0)


def gelu_parts(values):
    size = jnp.abs(values)
    step = 1.0 / (1.0 + (0.3275911 * 0.7071067811865476) * size)
    bell = jnp.exp(-0.5 * values * values)
    series = step * (
        0.5 * 0.254829592
        + step
        * (
            0.5 * -0.284496736
            + step * (0.5 * 1.421413741 + step * (0.5 * -1.453152027 + step * (0.5 * 1.061405429)))
        )
    )
    low = series * bell
    phi = jnp.where(values < 0.0, low, 1.0 - low)
    return values * phi, phi + values * (bell * 0.3989422804014327)


class Layout:
    def __init__(self, samples, rows_dev):
        self.samples = samples
        self.rows_dev = rows_dev
        self.n_dp = lax.axis_size("dp")
        self.n_wide = lax.axis_size("wide")
        self.parts = self.n_wide // samples
        self.pair = self.parts == 2 and self.n_dp % 2 == 0
        dp, wide = lax.axis_index("dp"), lax.axis_index("wide")
        self.turn = wide // self.parts
        self.part = dp % 2 if self.pair else wide % self.parts

    def shift(self, pieces, step):
        routes = []
        for dp in range(self.n_dp):
            for wide in range(self.n_wide):
                turn, part = divmod(wide, self.parts)
                goal = (turn + step) % self.samples
                if self.pair:
                    target = (dp // 2 * 2 + part) * self.n_wide + goal * 2 + dp % 2
                else:
                    target = dp * self.n_wide + goal * self.parts + part
                routes.append((dp * self.n_wide + wide, target))
        return lax.ppermute(pieces, AXES, routes)

    def rows_of(self, part):
        steps = jnp.arange(self.samples, dtype=jnp.int32)
        blocks = (self.turn - steps) % self.samples * self.parts + part
        inside = jnp.arange(self.rows_dev, dtype=jnp.int32)
        return (blocks[:, None] * self.rows_dev + inside[None, :]).reshape(-1)

    def orders(self, freqs):
        if self.pair:
            row_ids = jnp.concatenate([self.rows_of(self.part), self.rows_of(1 - self.part)])
            span = jnp.arange(freqs // 2, dtype=jnp.int32)
            freq_ids = jnp.concatenate(
                [self.part * (freqs // 2) + span, (1 - self.part) * (freqs // 2) + span]
            )
        else:
            row_ids = jnp.concatenate([self.rows_of(part) for part in range(self.parts)])
            freq_ids = jnp.arange(freqs, dtype=jnp.int32)
        return row_ids, freq_ids

    def swap(self, values):
        routes = []
        for dp in range(self.n_dp):
            for wide in range(self.n_wide):
                routes.append((dp * self.n_wide + wide, (dp ^ 1) * self.n_wide + wide))
        return lax.ppermute(values, AXES, routes)

    def groups(self):
        return [
            [turn * self.parts + part for part in range(self.parts)] for turn in range(self.samples)
        ]

    def to_freqs(self, rows):
        if self.pair:
            half = rows.shape[2] // 2
            arrived = self.swap(rows[:, :, half:])
            return jnp.concatenate([rows[:, :, :half], arrived], axis=0)
        return lax.all_to_all(
            rows, "wide", split_axis=2, concat_axis=0, axis_index_groups=self.groups(), tiled=True
        )

    def to_rows(self, cols):
        if self.pair:
            half = cols.shape[0] // 2
            arrived = self.swap(cols[half:])
            return jnp.concatenate([cols[:half], arrived], axis=2)
        return lax.all_to_all(
            cols, "wide", split_axis=0, concat_axis=2, axis_index_groups=self.groups(), tiled=True
        )


def make_tables(grid_height, grid_width, row_ids, freq_ids):
    across = jnp.arange(grid_width, dtype=jnp.int32)
    angles = (
        2.0 * jnp.pi / grid_width * (across[:, None] * freq_ids[None, :] % grid_width).astype(F32)
    )
    row_table = (
        jnp.stack([jnp.cos(angles), -jnp.sin(angles)], axis=1) / jnp.sqrt(F32(grid_width))
    ).astype(BF16)
    doubling = jnp.where(freq_ids == 0, 1.0, 2.0).astype(F32)
    inv_table = (row_table.astype(F32) * doubling).astype(BF16)
    down = jnp.arange(grid_height, dtype=jnp.int32)
    col_angles = (
        2.0 * jnp.pi / grid_height * (down[:, None] * row_ids[None, :] % grid_height).astype(F32)
    )
    cosine = jnp.cos(col_angles) / jnp.sqrt(F32(grid_height))
    sine = jnp.sin(col_angles) / jnp.sqrt(F32(grid_height))
    col_table = jnp.stack([jnp.stack([cosine, sine]), jnp.stack([-sine, cosine])]).astype(BF16)
    return row_table, inv_table, col_table


def bits_of(size):
    count = size.bit_length() - 1
    assert 1 << count == size
    return count


def route_bit(bit, total):
    return [(index, index ^ (1 << bit)) for index in range(total)]


def my_bit(bit):
    index = lax.axis_index("dp") * lax.axis_size("wide") + lax.axis_index("wide")
    return (index >> bit) & 1


def bit_orders():
    wide_bits = bits_of(lax.axis_size("wide"))
    dp_bits = bits_of(lax.axis_size("dp"))
    slow = list(range(wide_bits - 1, 0, -1))
    high = list(range(wide_bits + dp_bits - 1, wide_bits, -1))
    return slow + high + [0, wide_bits], slow + [0] + high + [wide_bits]


def gather_shards(shard, order):
    total = lax.axis_size("dp") * lax.axis_size("wide")
    held, have = shard, []
    for bit in order:
        arrived = lax.ppermute(held, AXES, route_bit(bit, total))
        place = sum(1 for other in have if other > bit)
        mine = my_bit(bit) == 1
        low, high = jnp.where(mine, arrived, held), jnp.where(mine, held, arrived)
        held = jnp.stack([low, high], axis=place)
        have.append(bit)
    return held.reshape((total * shard.shape[0],) + shard.shape[1:])


def scatter_sum(values, order):
    total = lax.axis_size("dp") * lax.axis_size("wide")
    count = bits_of(total)
    left = list(range(count - 1, -1, -1))
    held = values.reshape((2,) * count + (values.shape[0] // total, values.shape[1]))
    for bit in order:
        place = left.index(bit)
        mine = my_bit(bit)
        sent = lax.dynamic_index_in_dim(held, 1 - mine, place, keepdims=False).astype(BF16)
        kept = lax.dynamic_index_in_dim(held, mine, place, keepdims=False)
        arrived = lax.ppermute(sent, AXES, route_bit(bit, total))
        held = kept.astype(F32) + arrived.astype(F32)
        left.remove(bit)
        if left:
            held = held.astype(BF16)
    return held


def block_diagonal(weight):
    width, size = weight.shape
    block = jnp.arange(width, dtype=jnp.int32) // size
    return jnp.where(
        block[:, None] == block[None, :], jnp.tile(weight, (1, width // size)), jnp.zeros((), weight.dtype)
    )


def diagonal_blocks(cross, size):
    width = cross.shape[0]
    block = jnp.arange(width, dtype=jnp.int32) // size
    kept = jnp.where(block[:, None] == block[None, :], cross, 0.0)
    return sum(kept[:, start : start + size] for start in range(0, width, size))


def mix(spec, weight, bias):
    last = ((1,), (0,))
    real = dot(spec[0], weight[0], last) - dot(spec[1], weight[1], last) + bias[0]
    imag = dot(spec[0], weight[1], last) + dot(spec[1], weight[0], last) + bias[1]
    return real, imag


def mix_back(d_re, d_im, weight):
    last = ((1,), (1,))
    real = dot(d_re, weight[0], last) + dot(d_im, weight[1], last)
    imag = dot(d_im, weight[0], last) - dot(d_re, weight[1], last)
    return real, imag


def mix_weight(in_re, in_im, d_re, d_im, size):
    first = ((0,), (0,))
    real = dot(in_re, d_re, first) + dot(in_im, d_im, first)
    imag = dot(in_re, d_im, first) - dot(in_im, d_re, first)
    bias = jnp.stack([jnp.sum(d_re, axis=0, dtype=F32), jnp.sum(d_im, axis=0, dtype=F32)])
    return jnp.stack([diagonal_blocks(real, size), diagonal_blocks(imag, size)]), bias


def adam_update(master, moment, square, grad, factor, rate, decay):
    clipped = grad * factor
    moment_next = BETA_ONE * moment + (1.0 - BETA_ONE) * clipped
    square_next = BETA_TWO * square + (1.0 - BETA_TWO) * clipped * clipped
    ratio = (
        moment_next / (1.0 - BETA_ONE**10) / (jnp.sqrt(square_next / (1.0 - BETA_TWO**10)) + 1e-08)
    )
    return (master - rate * (ratio + decay * master), moment_next, square_next)


def shards(
    fields,
    targets,
    patch_mask,
    channel_mask,
    *state,
):
    masters, moments, squares = state[:6], state[6:12], state[12:]
    samples, rows_dev, grid_width, patch_dim = fields.shape
    layout = Layout(samples, rows_dev)
    grid_height = rows_dev * layout.n_wide
    channels = channel_mask.shape[1]
    pixels = patch_dim // channels
    rows = samples * rows_dev
    tokens = rows * grid_width
    freqs = grid_width // 2
    width_model = masters[0].shape[1]
    size = masters[4].shape[3]

    fields_sent, targets_sent = [], []
    for step in range(samples):
        sample = (layout.turn + step) % samples
        piece = lax.dynamic_index_in_dim(fields, sample, 0, keepdims=False)
        mask = lax.dynamic_index_in_dim(patch_mask, sample, 0, keepdims=False)
        fields_sent.append(piece * mask[..., None].astype(BF16))
        piece = lax.dynamic_index_in_dim(targets, sample, 0, keepdims=False)
        seen = lax.dynamic_index_in_dim(channel_mask, sample, 0, keepdims=False)
        seen = jnp.repeat(seen, pixels)
        used = (mask[..., None] * seen) > 0
        targets_sent.append(jnp.where(used, piece, jnp.asarray(UNUSED, BF16)))
    pieces = [layout.shift(piece, step) for step, piece in enumerate(fields_sent)]
    inputs = jnp.concatenate(pieces, axis=0).reshape(tokens, patch_dim)

    valid_patch = patch_mask.astype(F32)
    channel_on = channel_mask.astype(F32)
    local_counts = jnp.sum(channel_on * jnp.sum(valid_patch, axis=(1, 2))[:, None], axis=0) * pixels
    counts = lax.psum(local_counts, AXES)
    scale_cols = jnp.repeat(1.0 / (channels * counts), pixels)

    order_one, order_two = bit_orders()
    shard_rows = masters[4].shape[2]
    mixed = jnp.concatenate(
        [
            masters[4].transpose(2, 0, 1, 3).reshape(shard_rows, 4 * size),
            masters[5].T,
        ],
        axis=1,
    ).astype(BF16)
    mixed = jnp.pad(mixed, ((0, 0), (0, -mixed.shape[1] % 128)))
    embed_used = gather_shards(masters[0].astype(BF16), order_one)
    mixed_used = gather_shards(mixed, order_two)
    expand_used = gather_shards(masters[2].astype(BF16), order_one)
    project_used = gather_shards(masters[3].astype(BF16), order_two)
    head_used = gather_shards(masters[1].astype(BF16), order_two)
    small_used = mixed_used[:, 4 * size : 4 * size + 14].T.astype(F32)
    spectral_used = [
        [
            block_diagonal(mixed_used[:, (2 * layer + side) * size : (2 * layer + side + 1) * size])
            for side in range(2)
        ]
        for layer in range(2)
    ]

    targets_sent = lax.optimization_barrier((tuple(targets_sent), pieces[-1]))[0]
    goals = jnp.concatenate(
        [layout.shift(piece, step) for step, piece in enumerate(targets_sent)], axis=0
    ).reshape(tokens, patch_dim)

    row_ids, freq_ids = layout.orders(freqs)
    row_table, inv_table, col_table = make_tables(grid_height, grid_width, row_ids, freq_ids)

    hidden_zero = dot(inputs, embed_used, ((1,), (0,))) + small_used[4]
    unit_one, rstd_one = normalize(hidden_zero)
    normed_one = unit_one * small_used[0] + small_used[1]
    normed_low = normed_one.astype(BF16).reshape(rows, grid_width, width_model)
    rows_freq = jnp.einsum(
        "rwd,wak->rakd", normed_low, row_table, preferred_element_type=F32
    ).astype(BF16)
    rows_moved = layout.to_freqs(rows_freq)
    own_freqs = rows_moved.shape[2]
    spectrum = jnp.einsum(
        "oaxi,iakd->oxkd", col_table, rows_moved, preferred_element_type=F32
    ).astype(BF16)
    spectrum = spectrum.reshape(2, grid_height * own_freqs, width_model)
    first_pre = mix(spectrum, spectral_used[0], small_used[10:12])
    first_act = [jax.nn.relu(part).astype(BF16) for part in first_pre]
    second_pre = mix(first_act, spectral_used[1], small_used[12:14])
    shrunk = jnp.stack(
        [(part - jnp.clip(part, -SHRINK, SHRINK)).astype(BF16) for part in second_pre]
    ).reshape(2, grid_height, own_freqs, width_model)
    open_gate = [jnp.abs(part) > SHRINK for part in second_pre]
    back_cols = jnp.einsum(
        "aoxi,axkd->iokd", col_table, shrunk, preferred_element_type=F32
    ).astype(BF16)
    cols_moved = layout.to_rows(back_cols)
    filtered = jnp.einsum(
        "wak,rakd->rwd", inv_table, cols_moved, preferred_element_type=F32
    ).reshape(tokens, width_model)
    hidden_one = hidden_zero + filtered + normed_one
    unit_two, rstd_two = normalize(hidden_one)
    normed_two = (unit_two * small_used[2] + small_used[3]).astype(BF16)
    expand_pre = dot(normed_two, expand_used, ((1,), (0,))) + small_used[6:10].reshape(-1)
    expand_act, gelu_slope = gelu_parts(expand_pre)
    expand_act = expand_act.astype(BF16)
    hidden_two = hidden_one + dot(expand_act, project_used, ((1,), (0,))) + small_used[5]
    hidden_low = hidden_two.astype(BF16)
    predict = dot(hidden_low, head_used, ((1,), (0,)))

    goals = goals.astype(F32)
    errors = jnp.where(goals < 0.5 * UNUSED, predict - goals, 0.0)
    column_errors = jnp.sum(errors * errors, axis=0)
    grad_low = (2.0 * errors * scale_cols).astype(BF16)

    order_sum_one, order_sum_two = order_one[::-1], order_two[::-1]
    grad_head = dot(hidden_low, grad_low, ((0,), (0,))).astype(BF16)
    reduced_head = scatter_sum(grad_head, order_sum_two)
    grad_two = dot(grad_low, head_used, ((1,), (1,)))
    grad_branch = grad_two.astype(BF16)
    grad_project = dot(expand_act, grad_branch, ((0,), (0,))).astype(BF16)
    reduced_project = scatter_sum(grad_project, order_sum_two)
    bias_project = jnp.sum(grad_branch, axis=0, dtype=F32)
    grad_act = dot(grad_branch, project_used, ((1,), (1,)))
    grad_pre = (grad_act * gelu_slope).astype(BF16)
    grad_expand = dot(normed_two, grad_pre, ((0,), (0,))).astype(BF16)
    reduced_expand = scatter_sum(grad_expand, order_sum_one)
    bias_expand = jnp.sum(grad_pre, axis=0, dtype=F32)
    grad_normed = dot(grad_pre, expand_used, ((1,), (1,)))
    back_one, gain_two, shift_two = norm_back(grad_normed, unit_two, rstd_two, small_used[2])
    grad_one = grad_two + back_one
    grad_filter = grad_one.astype(BF16).reshape(rows, grid_width, width_model)
    grad_cols = jnp.einsum(
        "wak,rwd->rakd", inv_table, grad_filter, preferred_element_type=F32
    ).astype(BF16)
    grad_moved = layout.to_freqs(grad_cols)
    grad_shrunk = jnp.einsum(
        "aoxi,iokd->axkd", col_table, grad_moved, preferred_element_type=F32
    ).reshape(2, grid_height * own_freqs, width_model)
    d_second = [
        jnp.where(open_gate[side], grad_shrunk[side], 0.0).astype(BF16) for side in range(2)
    ]
    grad_first_act = mix_back(*d_second, spectral_used[1])
    weight_two, bias_two = mix_weight(*first_act, *d_second, size)
    d_first = [
        jnp.where(first_pre[side] > 0.0, grad_first_act[side], 0.0).astype(BF16)
        for side in range(2)
    ]
    grad_spectrum = mix_back(*d_first, spectral_used[0])
    weight_one, bias_one = mix_weight(spectrum[0], spectrum[1], *d_first, size)
    grad_spectrum = jnp.stack([part.astype(BF16) for part in grad_spectrum]).reshape(
        2, grid_height, own_freqs, width_model
    )
    grad_rows = jnp.einsum(
        "oaxi,oxkd->iakd", col_table, grad_spectrum, preferred_element_type=F32
    ).astype(BF16)
    grad_back = layout.to_rows(grad_rows)
    grad_normed_one = (
        jnp.einsum("wak,rakd->rwd", row_table, grad_back, preferred_element_type=F32).reshape(
            tokens, width_model
        )
        + grad_one
    )
    back_zero, gain_one, shift_one = norm_back(grad_normed_one, unit_one, rstd_one, small_used[0])
    grad_zero = (grad_one + back_zero).astype(BF16)
    grad_embed = dot(inputs, grad_zero, ((0,), (0,))).astype(BF16)
    reduced_embed = scatter_sum(grad_embed, order_sum_one)
    bias_embed = jnp.sum(grad_zero, axis=0, dtype=F32)
    grad_small = jnp.concatenate(
        [
            jnp.stack([gain_one, shift_one, gain_two, shift_two, bias_embed, bias_project]),
            bias_expand.reshape(4, width_model),
            bias_one,
            bias_two,
        ],
        axis=0,
    )
    grad_mixed = jnp.concatenate(
        [weight_one[0], weight_one[1], weight_two[0], weight_two[1], grad_small.T], axis=1
    )
    grad_mixed = jnp.pad(grad_mixed, ((0, 0), (0, -grad_mixed.shape[1] % 128)))
    reduced_mixed = scatter_sum(grad_mixed, order_sum_two)
    reduced_spectral = (
        reduced_mixed[:, : 4 * size].reshape(shard_rows, 2, 2, size).transpose(1, 2, 0, 3)
    )
    reduced_small = reduced_mixed[:, 4 * size : 4 * size + 14].T
    reduced = (
        reduced_embed,
        reduced_head,
        reduced_expand,
        reduced_project,
        reduced_spectral,
        reduced_small,
    )

    local_square = sum(jnp.sum(grad * grad) for grad in reduced)
    local_error = jnp.sum(column_errors.reshape(channels, pixels), axis=1)
    total_square, error_sums = lax.psum((local_square, local_error), AXES)
    grad_norm = jnp.sqrt(total_square)
    loss = jnp.sum(error_sums / counts) / channels
    batch = samples * layout.n_dp
    clip_level = 0.25 / jnp.sqrt(F32(batch * grid_height * grid_width))
    factor = jnp.minimum(1.0, clip_level / grad_norm)
    results = [loss, grad_norm]
    for index in range(6):
        results.extend(
            adam_update(
                masters[index],
                moments[index],
                squares[index],
                reduced[index],
                factor,
                RATES[index],
                DECAYS[index],
            )
        )
    return tuple(results)


def solution(mesh):
    placed = (
        P("dp", "wide", None, None),
        P("dp", "wide", None, None),
        P("dp", "wide", None),
        P("dp", None),
        P(("dp", "wide"), None),
        P(("dp", "wide"), None),
        P(("dp", "wide"), None),
        P(("dp", "wide"), None),
        P(None, None, ("dp", "wide"), None),
        P(None, ("dp", "wide")),
        P(("dp", "wide"), None),
        P(("dp", "wide"), None),
        P(("dp", "wide"), None),
        P(("dp", "wide"), None),
        P(None, None, ("dp", "wide"), None),
        P(None, ("dp", "wide")),
        P(("dp", "wide"), None),
        P(("dp", "wide"), None),
        P(("dp", "wide"), None),
        P(("dp", "wide"), None),
        P(None, None, ("dp", "wide"), None),
        P(None, ("dp", "wide")),
    )
    return jax.shard_map(
        shards,
        mesh=mesh,
        in_specs=placed,
        out_specs=(
            P(),
            P(),
            P(("dp", "wide"), None),
            P(("dp", "wide"), None),
            P(("dp", "wide"), None),
            P(("dp", "wide"), None),
            P(("dp", "wide"), None),
            P(("dp", "wide"), None),
            P(("dp", "wide"), None),
            P(("dp", "wide"), None),
            P(("dp", "wide"), None),
            P(("dp", "wide"), None),
            P(("dp", "wide"), None),
            P(("dp", "wide"), None),
            P(None, None, ("dp", "wide"), None),
            P(None, None, ("dp", "wide"), None),
            P(None, None, ("dp", "wide"), None),
            P(None, ("dp", "wide")),
            P(None, ("dp", "wide")),
            P(None, ("dp", "wide")),
        ),
        check_vma=False,
    )
```

```python
import jax
import jax.numpy as jnp
from jax import lax
from jax.experimental import pallas as pl
from jax.experimental.pallas import tpu as pltpu
from jax.sharding import PartitionSpec as P

EPSILON = 1e-06
SHRINK = 0.01
BETA_ONE = 0.9
BETA_TWO = 0.95
RATES = (0.08, 0.1, 0.1, 0.05, 0.3, 0.5)
DECAYS = (0.1, 0.1, 0.1, 0.1, 0.1, 0.0)
AXES = ("dp", "wide")
UNUSED = 64.0
BF16 = jnp.bfloat16
F32 = jnp.float32


def dot(left, right, dims):
    return lax.dot_general(left, right, (dims, ((), ())), preferred_element_type=F32)


def normalize(values):
    centred = values - jnp.mean(values, axis=-1, keepdims=True)
    spread = jnp.mean(centred * centred, axis=-1, keepdims=True)
    rstd = lax.rsqrt(spread + EPSILON)
    return centred * rstd, rstd


def norm_back(grad, unit, rstd, gain):
    scaled = grad * gain
    first = jnp.mean(scaled, axis=-1, keepdims=True)
    second = jnp.mean(scaled * unit, axis=-1, keepdims=True)
    back = rstd * (scaled - first - unit * second)
    return back, jnp.sum(grad * unit, axis=0), jnp.sum(grad, axis=0)


def gelu_parts(values):
    size = jnp.abs(values)
    step = 1.0 / (1.0 + (0.3275911 * 0.7071067811865476) * size)
    bell = jnp.exp(-0.5 * values * values)
    series = step * (
        0.5 * 0.254829592
        + step
        * (
            0.5 * -0.284496736
            + step * (0.5 * 1.421413741 + step * (0.5 * -1.453152027 + step * (0.5 * 1.061405429)))
        )
    )
    low = series * bell
    phi = jnp.where(values < 0.0, low, 1.0 - low)
    return values * phi, phi + values * (bell * 0.3989422804014327)


class Layout:
    def __init__(self, samples, rows_dev):
        self.samples = samples
        self.rows_dev = rows_dev
        self.n_dp = lax.axis_size("dp")
        self.n_wide = lax.axis_size("wide")
        self.parts = self.n_wide // samples
        self.pair = self.parts == 2 and self.n_dp % 2 == 0
        dp, wide = lax.axis_index("dp"), lax.axis_index("wide")
        self.turn = wide // self.parts
        self.part = dp % 2 if self.pair else wide % self.parts

    def shift(self, pieces, step):
        if step == 0 and not self.pair:
            return pieces
        routes, same = [], []
        for dp in range(self.n_dp):
            for wide in range(self.n_wide):
                turn, part = divmod(wide, self.parts)
                goal = (turn + step) % self.samples
                if self.pair:
                    target = (dp // 2 * 2 + part) * self.n_wide + goal * 2 + dp % 2
                else:
                    target = dp * self.n_wide + goal * self.parts + part
                source = dp * self.n_wide + wide
                if source == target:
                    same.append(source)
                else:
                    routes.append((source, target))
        arrived = lax.ppermute(pieces, AXES, routes)
        if same:
            stays = lax.axis_index("dp") % 2 == lax.axis_index("wide") % self.parts
            arrived = jnp.where(stays, pieces, arrived)
        return arrived

    def rows_of(self, part):
        steps = jnp.arange(self.samples, dtype=jnp.int32)
        blocks = (self.turn - steps) % self.samples * self.parts + part
        inside = jnp.arange(self.rows_dev, dtype=jnp.int32)
        return (blocks[:, None] * self.rows_dev + inside[None, :]).reshape(-1)

    def orders(self, freqs):
        if self.pair:
            row_ids = jnp.concatenate([self.rows_of(self.part), self.rows_of(1 - self.part)])
            span = jnp.arange(freqs // 2, dtype=jnp.int32)
            freq_ids = jnp.concatenate(
                [self.part * (freqs // 2) + span, (1 - self.part) * (freqs // 2) + span]
            )
        else:
            row_ids = jnp.concatenate([self.rows_of(part) for part in range(self.parts)])
            freq_ids = jnp.arange(freqs, dtype=jnp.int32)
        return row_ids, freq_ids

    def swap(self, values):
        routes = []
        for dp in range(self.n_dp):
            for wide in range(self.n_wide):
                routes.append((dp * self.n_wide + wide, (dp ^ 1) * self.n_wide + wide))
        return lax.ppermute(values, AXES, routes)

    def groups(self):
        return [
            [turn * self.parts + part for part in range(self.parts)] for turn in range(self.samples)
        ]

    def to_freqs(self, rows):
        if self.pair:
            half = rows.shape[2] // 2
            arrived = self.swap(rows[:, :, half:])
            return jnp.concatenate([rows[:, :, :half], arrived], axis=0)
        return lax.all_to_all(
            rows, "wide", split_axis=2, concat_axis=0, axis_index_groups=self.groups(), tiled=True
        )

    def to_rows(self, cols):
        if self.pair:
            half = cols.shape[0] // 2
            arrived = self.swap(cols[half:])
            return jnp.concatenate([cols[:half], arrived], axis=2)
        return lax.all_to_all(
            cols, "wide", split_axis=0, concat_axis=2, axis_index_groups=self.groups(), tiled=True
        )


def make_tables(grid_height, grid_width, row_ids, freq_ids):
    across = jnp.arange(grid_width, dtype=jnp.int32)
    angles = (
        2.0 * jnp.pi / grid_width * (across[:, None] * freq_ids[None, :] % grid_width).astype(F32)
    )
    row_table = (
        jnp.stack([jnp.cos(angles), -jnp.sin(angles)], axis=1) / jnp.sqrt(F32(grid_width))
    ).astype(BF16)
    doubling = jnp.where(freq_ids == 0, 1.0, 2.0).astype(F32)
    inv_table = (row_table.astype(F32) * doubling).astype(BF16)
    down = jnp.arange(grid_height, dtype=jnp.int32)
    col_angles = (
        2.0 * jnp.pi / grid_height * (down[:, None] * row_ids[None, :] % grid_height).astype(F32)
    )
    cosine = jnp.cos(col_angles) / jnp.sqrt(F32(grid_height))
    sine = jnp.sin(col_angles) / jnp.sqrt(F32(grid_height))
    col_table = jnp.stack([jnp.stack([cosine, sine]), jnp.stack([-sine, cosine])]).astype(BF16)
    return row_table, inv_table, col_table


def bits_of(size):
    count = size.bit_length() - 1
    assert 1 << count == size
    return count


def route_bit(bit, total):
    return [(index, index ^ (1 << bit)) for index in range(total)]


def my_bit(bit):
    index = lax.axis_index("dp") * lax.axis_size("wide") + lax.axis_index("wide")
    return (index >> bit) & 1


def bit_orders():
    wide_bits = bits_of(lax.axis_size("wide"))
    dp_bits = bits_of(lax.axis_size("dp"))
    slow = list(range(wide_bits - 1, 0, -1))
    high = list(range(wide_bits + dp_bits - 1, wide_bits, -1))
    return slow + high + [0, wide_bits], slow + [0] + high + [wide_bits]


def gather_shards(shard, order):
    total = lax.axis_size("dp") * lax.axis_size("wide")
    held, have = shard, []
    for bit in order:
        arrived = lax.ppermute(held, AXES, route_bit(bit, total))
        place = sum(1 for other in have if other > bit)
        mine = my_bit(bit) == 1
        low, high = jnp.where(mine, arrived, held), jnp.where(mine, held, arrived)
        held = jnp.stack([low, high], axis=place)
        have.append(bit)
    return held.reshape((total * shard.shape[0],) + shard.shape[1:])


class Halving:
    def __init__(self, values, order):
        self.total = lax.axis_size("dp") * lax.axis_size("wide")
        count = bits_of(self.total)
        self.left = list(range(count - 1, -1, -1))
        self.order = list(order)
        self.held = values.reshape((2,) * count + (values.shape[0] // self.total, values.shape[1]))
        self.send()

    def send(self):
        bit = self.order.pop(0)
        place = self.left.index(bit)
        mine = my_bit(bit)
        sent = lax.dynamic_index_in_dim(self.held, 1 - mine, place, keepdims=False).astype(BF16)
        self.kept = lax.dynamic_index_in_dim(self.held, mine, place, keepdims=False)
        self.arrived = lax.ppermute(sent, AXES, route_bit(bit, self.total))
        self.left.remove(bit)

    def step(self):
        self.held = self.kept.astype(F32) + self.arrived.astype(F32)
        if self.order:
            self.held = self.held.astype(BF16)
            self.send()

    def finish(self):
        while self.order:
            self.step()
        self.step()
        return self.held


def advance(running, anchor):
    if not running[0].order:
        return anchor
    arrived, anchor = lax.optimization_barrier((tuple(one.arrived for one in running), anchor))
    for one, value in zip(running, arrived):
        one.arrived = value
        one.step()
    return anchor


def sum_kernel(n_dp, n_wide, mine_ref, out_ref, box, own_sem, send_sem, recv_sem):
    total = n_dp * n_wide
    me = lax.axis_index("dp") * n_wide + lax.axis_index("wide")

    def place(index):
        return (index // n_wide, index % n_wide)

    def push(offset):
        return pltpu.make_async_remote_copy(
            src_ref=mine_ref,
            dst_ref=box.at[me],
            send_sem=send_sem.at[offset],
            recv_sem=recv_sem.at[me],
            device_id=place((me + offset) % total),
            device_id_type=pl.DeviceIdType.MESH,
        )

    def pull(offset):
        source = (me + total - offset) % total
        return pltpu.make_async_remote_copy(
            src_ref=mine_ref,
            dst_ref=box.at[source],
            send_sem=send_sem.at[offset],
            recv_sem=recv_sem.at[source],
            device_id=place(source),
            device_id_type=pl.DeviceIdType.MESH,
        )

    barrier = pltpu.get_barrier_semaphore()

    @pl.loop(1, total)
    def _(offset):
        pl.semaphore_signal(
            barrier, inc=1, device_id=place((me + offset) % total), device_id_type=pl.DeviceIdType.MESH
        )

    own = pltpu.make_async_copy(mine_ref, box.at[me], own_sem)
    own.start()
    pl.semaphore_wait(barrier, total - 1)

    @pl.loop(1, total)
    def _(offset):
        push(offset).start()

    own.wait()

    @pl.loop(1, total)
    def _(offset):
        push(offset).wait_send()
        pull(offset).wait_recv()

    out_ref[...] = jnp.sum(box[...], axis=0)


def sum_everywhere(values):
    n_dp, n_wide = lax.axis_size("dp"), lax.axis_size("wide")
    total = n_dp * n_wide

    def kernel(*refs):
        sum_kernel(n_dp, n_wide, *refs)

    return pl.pallas_call(
        kernel,
        out_shape=jax.ShapeDtypeStruct(values.shape, F32),
        in_specs=[pl.BlockSpec(memory_space=pltpu.VMEM)],
        out_specs=pl.BlockSpec(memory_space=pltpu.VMEM),
        scratch_shapes=[
            pltpu.VMEM((total,) + values.shape, F32),
            pltpu.SemaphoreType.DMA,
            pltpu.SemaphoreType.DMA((total,)),
            pltpu.SemaphoreType.DMA((total,)),
        ],
        compiler_params=pltpu.CompilerParams(collective_id=3, has_side_effects=True),
        name="sum_everywhere",
    )(values)


def join(pieces):
    whole = jnp.zeros((len(pieces),) + pieces[0].shape, pieces[0].dtype)
    for place, piece in enumerate(pieces):
        whole = whole.at[place].set(piece)
    return whole


def block_diagonal(weight):
    width, size = weight.shape
    block = jnp.arange(width, dtype=jnp.int32) // size
    return jnp.where(
        block[:, None] == block[None, :], jnp.tile(weight, (1, width // size)), jnp.zeros((), weight.dtype)
    )


def diagonal_blocks(cross, size):
    width = cross.shape[0]
    block = jnp.arange(width, dtype=jnp.int32) // size
    kept = jnp.where(block[:, None] == block[None, :], cross, 0.0)
    return sum(kept[:, start : start + size] for start in range(0, width, size))


def mix(spec, weight, bias):
    last = ((1,), (0,))
    real = dot(spec[0], weight[0], last) - dot(spec[1], weight[1], last) + bias[0]
    imag = dot(spec[0], weight[1], last) + dot(spec[1], weight[0], last) + bias[1]
    return real, imag


def mix_back(d_re, d_im, weight):
    last = ((1,), (1,))
    real = dot(d_re, weight[0], last) + dot(d_im, weight[1], last)
    imag = dot(d_im, weight[0], last) - dot(d_re, weight[1], last)
    return real, imag


def mix_weight(in_re, in_im, d_re, d_im, size):
    first = ((0,), (0,))
    real = dot(in_re, d_re, first) + dot(in_im, d_im, first)
    imag = dot(in_re, d_im, first) - dot(in_im, d_re, first)
    bias = jnp.stack([jnp.sum(d_re, axis=0, dtype=F32), jnp.sum(d_im, axis=0, dtype=F32)])
    return jnp.stack([diagonal_blocks(real, size), diagonal_blocks(imag, size)]), bias


def adam_update(master, moment, square, grad, factor, rate, decay):
    clipped = grad * factor
    moment_next = BETA_ONE * moment + (1.0 - BETA_ONE) * clipped
    square_next = BETA_TWO * square + (1.0 - BETA_TWO) * clipped * clipped
    ratio = (
        moment_next / (1.0 - BETA_ONE**10) / (jnp.sqrt(square_next / (1.0 - BETA_TWO**10)) + 1e-08)
    )
    return (master - rate * (ratio + decay * master), moment_next, square_next)


def shards(
    fields,
    targets,
    patch_mask,
    channel_mask,
    *state,
):
    masters, moments, squares = state[:6], state[6:12], state[12:]
    samples, rows_dev, grid_width, patch_dim = fields.shape
    layout = Layout(samples, rows_dev)
    grid_height = rows_dev * layout.n_wide
    channels = channel_mask.shape[1]
    pixels = patch_dim // channels
    rows = samples * rows_dev
    tokens = rows * grid_width
    freqs = grid_width // 2
    width_model = masters[0].shape[1]
    size = masters[4].shape[3]

    fields_sent, targets_sent = [], []
    for step in range(samples):
        sample = (layout.turn + step) % samples
        piece = lax.dynamic_index_in_dim(fields, sample, 0, keepdims=False)
        mask = lax.dynamic_index_in_dim(patch_mask, sample, 0, keepdims=False)
        fields_sent.append(piece * mask[..., None].astype(BF16))
        piece = lax.dynamic_index_in_dim(targets, sample, 0, keepdims=False)
        seen = lax.dynamic_index_in_dim(channel_mask, sample, 0, keepdims=False)
        seen = jnp.repeat(seen, pixels)
        used = (mask[..., None] * seen) > 0
        targets_sent.append(jnp.where(used, piece, jnp.asarray(UNUSED, BF16)))
    pieces = [layout.shift(piece, step) for step, piece in enumerate(fields_sent)]
    inputs = join(pieces).reshape(tokens, patch_dim)

    valid_patch = patch_mask.astype(F32)
    channel_on = channel_mask.astype(F32)
    local_counts = jnp.sum(channel_on * jnp.sum(valid_patch, axis=(1, 2))[:, None], axis=0)
    upper = jnp.floor(local_counts / 256.0)
    digits = jnp.stack([upper, local_counts - 256.0 * upper])

    order_one, order_two = bit_orders()
    shard_rows = masters[4].shape[2]
    mixed = jnp.concatenate(
        [
            masters[4].transpose(2, 0, 1, 3).reshape(shard_rows, 4 * size),
            masters[5].T,
            jnp.pad(digits, ((0, shard_rows - 2), (0, 0))),
        ],
        axis=1,
    ).astype(BF16)
    mixed = jnp.pad(mixed, ((0, 0), (0, -mixed.shape[1] % 128)))
    embed_used = gather_shards(masters[0].astype(BF16), order_one)
    mixed_used = gather_shards(mixed, order_two)
    expand_used = gather_shards(masters[2].astype(BF16), order_one)
    project_used = gather_shards(masters[3].astype(BF16), order_two)
    head_used = gather_shards(masters[1].astype(BF16), order_two)
    digits = mixed_used[:, 4 * size + 14 : 4 * size + 14 + channels].astype(F32)
    digits = jnp.sum(digits.reshape(-1, shard_rows, channels), axis=0)
    counts = (256.0 * digits[0] + digits[1]) * pixels
    scale_cols = jnp.repeat(1.0 / (channels * counts), pixels)
    small_used = mixed_used[:, 4 * size : 4 * size + 14].T.astype(F32)
    spectral_used = [
        [
            block_diagonal(mixed_used[:, (2 * layer + side) * size : (2 * layer + side + 1) * size])
            for side in range(2)
        ]
        for layer in range(2)
    ]

    targets_sent = lax.optimization_barrier((tuple(targets_sent), pieces[-1]))[0]
    goals = [layout.shift(piece, step) for step, piece in enumerate(targets_sent)]

    row_ids, freq_ids = layout.orders(freqs)
    row_table, inv_table, col_table = make_tables(grid_height, grid_width, row_ids, freq_ids)

    hidden_zero = dot(inputs, embed_used, ((1,), (0,))) + small_used[4]
    unit_one, rstd_one = normalize(hidden_zero)
    normed_one = unit_one * small_used[0] + small_used[1]
    normed_low = normed_one.astype(BF16).reshape(rows, grid_width, width_model)
    rows_freq = jnp.einsum(
        "rwd,wak->rakd", normed_low, row_table, preferred_element_type=F32
    ).astype(BF16)
    rows_moved = layout.to_freqs(rows_freq)
    own_freqs = rows_moved.shape[2]
    spectrum = jnp.einsum(
        "oaxi,iakd->oxkd", col_table, rows_moved, preferred_element_type=F32
    ).astype(BF16)
    spectrum = spectrum.reshape(2, grid_height * own_freqs, width_model)
    first_pre = mix(spectrum, spectral_used[0], small_used[10:12])
    first_act = [jax.nn.relu(part).astype(BF16) for part in first_pre]
    second_pre = mix(first_act, spectral_used[1], small_used[12:14])
    shrunk = jnp.stack(
        [(part - jnp.clip(part, -SHRINK, SHRINK)).astype(BF16) for part in second_pre]
    ).reshape(2, grid_height, own_freqs, width_model)
    open_gate = [jnp.abs(part) > SHRINK for part in second_pre]
    back_cols = jnp.einsum(
        "aoxi,axkd->iokd", col_table, shrunk, preferred_element_type=F32
    ).astype(BF16)
    cols_moved = layout.to_rows(back_cols)
    filtered = jnp.einsum(
        "wak,rakd->rwd", inv_table, cols_moved, preferred_element_type=F32
    ).reshape(tokens, width_model)
    hidden_one = hidden_zero + filtered + normed_one
    unit_two, rstd_two = normalize(hidden_one)
    normed_two = (unit_two * small_used[2] + small_used[3]).astype(BF16)
    expand_pre = dot(normed_two, expand_used, ((1,), (0,))) + small_used[6:10].reshape(-1)
    expand_act, gelu_slope = gelu_parts(expand_pre)
    expand_act, gelu_slope = lax.optimization_barrier(
        (expand_act.astype(BF16), gelu_slope.astype(BF16))
    )
    hidden_two = hidden_one + dot(expand_act, project_used, ((1,), (0,))) + small_used[5]
    hidden_low, goals = lax.optimization_barrier((hidden_two.astype(BF16), tuple(goals)))
    goals = join(goals).reshape(tokens, patch_dim)
    predict = dot(hidden_low, head_used, ((1,), (0,)))

    goals = goals.astype(F32)
    errors = jnp.where(goals < 0.5 * UNUSED, predict - goals, 0.0)
    column_errors = jnp.sum(errors * errors, axis=0)
    grad_low = (2.0 * errors * scale_cols).astype(BF16)

    order_sum_one, order_sum_two = order_one[::-1], order_two[::-1]
    grad_head = dot(hidden_low, grad_low, ((0,), (0,))).astype(BF16)
    sum_head = Halving(grad_head, order_sum_two)
    grad_two = dot(grad_low, head_used, ((1,), (1,)))
    grad_branch = grad_two.astype(BF16)
    grad_project = dot(expand_act, grad_branch, ((0,), (0,))).astype(BF16)
    sum_project = Halving(grad_project, order_sum_two)
    bias_project = jnp.sum(grad_branch, axis=0, dtype=F32)
    grad_act = dot(grad_branch, project_used, ((1,), (1,)))
    grad_pre = (grad_act * gelu_slope).astype(BF16)
    grad_expand = dot(normed_two, grad_pre, ((0,), (0,))).astype(BF16)
    sum_expand = Halving(grad_expand, order_sum_one)
    early = [sum_head, sum_project, sum_expand]
    bias_expand = jnp.sum(grad_pre, axis=0, dtype=F32)
    grad_normed = dot(grad_pre, expand_used, ((1,), (1,)))
    back_one, gain_two, shift_two = norm_back(grad_normed, unit_two, rstd_two, small_used[2])
    grad_one = grad_two + back_one
    grad_filter = grad_one.astype(BF16).reshape(rows, grid_width, width_model)
    grad_cols = jnp.einsum(
        "wak,rwd->rakd", inv_table, grad_filter, preferred_element_type=F32
    ).astype(BF16)
    grad_cols = advance(early, grad_cols)
    grad_moved = layout.to_freqs(grad_cols)
    grad_shrunk = jnp.einsum(
        "aoxi,iokd->axkd", col_table, grad_moved, preferred_element_type=F32
    ).reshape(2, grid_height * own_freqs, width_model)
    d_second = [
        jnp.where(open_gate[side], grad_shrunk[side], 0.0).astype(BF16) for side in range(2)
    ]
    d_second = advance(early, tuple(d_second))
    grad_first_act = mix_back(*d_second, spectral_used[1])
    weight_two, bias_two = mix_weight(*first_act, *d_second, size)
    d_first = [
        jnp.where(first_pre[side] > 0.0, grad_first_act[side], 0.0).astype(BF16)
        for side in range(2)
    ]
    d_first = advance(early, tuple(d_first))
    grad_spectrum = mix_back(*d_first, spectral_used[0])
    weight_one, bias_one = mix_weight(spectrum[0], spectrum[1], *d_first, size)
    grad_spectrum = jnp.stack([part.astype(BF16) for part in grad_spectrum]).reshape(
        2, grid_height, own_freqs, width_model
    )
    grad_rows = jnp.einsum(
        "oaxi,oxkd->iakd", col_table, grad_spectrum, preferred_element_type=F32
    ).astype(BF16)
    grad_rows = advance(early, grad_rows)
    grad_back = layout.to_rows(grad_rows)
    grad_normed_one = (
        jnp.einsum("wak,rakd->rwd", row_table, grad_back, preferred_element_type=F32).reshape(
            tokens, width_model
        )
        + grad_one
    )
    back_zero, gain_one, shift_one = norm_back(grad_normed_one, unit_one, rstd_one, small_used[0])
    grad_zero = (grad_one + back_zero).astype(BF16)
    grad_embed = dot(inputs, grad_zero, ((0,), (0,))).astype(BF16)
    reduced_embed = Halving(grad_embed, order_sum_one).finish()
    reduced_head, reduced_project, reduced_expand = [one.finish() for one in early]
    bias_embed = jnp.sum(grad_zero, axis=0, dtype=F32)
    grad_small = jnp.concatenate(
        [
            jnp.stack([gain_one, shift_one, gain_two, shift_two, bias_embed, bias_project]),
            bias_expand.reshape(4, width_model),
            bias_one,
            bias_two,
        ],
        axis=0,
    )
    grad_mixed = jnp.concatenate(
        [weight_one[0], weight_one[1], weight_two[0], weight_two[1], grad_small.T], axis=1
    )
    grad_mixed = jnp.pad(grad_mixed, ((0, 0), (0, -grad_mixed.shape[1] % 128)))
    reduced_mixed = Halving(grad_mixed, order_sum_two).finish()
    reduced_spectral = (
        reduced_mixed[:, : 4 * size].reshape(shard_rows, 2, 2, size).transpose(1, 2, 0, 3)
    )
    reduced_small = reduced_mixed[:, 4 * size : 4 * size + 14].T
    reduced = (
        reduced_embed,
        reduced_head,
        reduced_expand,
        reduced_project,
        reduced_spectral,
        reduced_small,
    )

    local_square = sum(jnp.sum(grad * grad) for grad in reduced)
    local_error = jnp.sum(column_errors.reshape(channels, pixels), axis=1)
    local_sums = jnp.concatenate([local_error, local_square[None]])
    sums = sum_everywhere(jnp.zeros((8, 128), F32).at[0, : channels + 1].set(local_sums))
    error_sums, total_square = sums[0, :channels], sums[0, channels]
    grad_norm = jnp.sqrt(total_square)
    loss = jnp.sum(error_sums / counts) / channels
    batch = samples * layout.n_dp
    clip_level = 0.25 / jnp.sqrt(F32(batch * grid_height * grid_width))
    factor = jnp.minimum(1.0, clip_level / grad_norm)
    results = [loss, grad_norm]
    for index in range(6):
        results.extend(
            adam_update(
                masters[index],
                moments[index],
                squares[index],
                reduced[index],
                factor,
                RATES[index],
                DECAYS[index],
            )
        )
    return tuple(results)


def solution(mesh):
    placed = (
        P("dp", "wide", None, None),
        P("dp", "wide", None, None),
        P("dp", "wide", None),
        P("dp", None),
        P(("dp", "wide"), None),
        P(("dp", "wide"), None),
        P(("dp", "wide"), None),
        P(("dp", "wide"), None),
        P(None, None, ("dp", "wide"), None),
        P(None, ("dp", "wide")),
        P(("dp", "wide"), None),
        P(("dp", "wide"), None),
        P(("dp", "wide"), None),
        P(("dp", "wide"), None),
        P(None, None, ("dp", "wide"), None),
        P(None, ("dp", "wide")),
        P(("dp", "wide"), None),
        P(("dp", "wide"), None),
        P(("dp", "wide"), None),
        P(("dp", "wide"), None),
        P(None, None, ("dp", "wide"), None),
        P(None, ("dp", "wide")),
    )
    return jax.shard_map(
        shards,
        mesh=mesh,
        in_specs=placed,
        out_specs=(
            P(),
            P(),
            P(("dp", "wide"), None),
            P(("dp", "wide"), None),
            P(("dp", "wide"), None),
            P(("dp", "wide"), None),
            P(("dp", "wide"), None),
            P(("dp", "wide"), None),
            P(("dp", "wide"), None),
            P(("dp", "wide"), None),
            P(("dp", "wide"), None),
            P(("dp", "wide"), None),
            P(("dp", "wide"), None),
            P(("dp", "wide"), None),
            P(None, None, ("dp", "wide"), None),
            P(None, None, ("dp", "wide"), None),
            P(None, None, ("dp", "wide"), None),
            P(None, ("dp", "wide")),
            P(None, ("dp", "wide")),
            P(None, ("dp", "wide")),
        ),
        check_vma=False,
    )
```

```python
import jax
import jax.numpy as jnp
from jax import lax
from jax.experimental import pallas as pl
from jax.experimental.pallas import tpu as pltpu
from jax.sharding import PartitionSpec as P


EPSILON = 1e-06
SHRINK = 0.01
BETA_ONE = 0.9
BETA_TWO = 0.95
RATES = (0.08, 0.1, 0.1, 0.05, 0.3, 0.5)
DECAYS = (0.1, 0.1, 0.1, 0.1, 0.1, 0.0)
AXES = ("dp", "wide")
UNUSED = 64.0
BF16 = jnp.bfloat16
F32 = jnp.float32


def dot(left, right, dims):
    return lax.dot_general(left, right, (dims, ((), ())), preferred_element_type=F32)


def normalize(values):
    centred = values - jnp.mean(values, axis=-1, keepdims=True)
    spread = jnp.mean(centred * centred, axis=-1, keepdims=True)
    rstd = lax.rsqrt(spread + EPSILON)
    return centred * rstd, rstd


def norm_back(grad, unit, rstd, gain):
    scaled = grad * gain
    first = jnp.mean(scaled, axis=-1, keepdims=True)
    second = jnp.mean(scaled * unit, axis=-1, keepdims=True)
    back = rstd * (scaled - first - unit * second)
    return back, jnp.sum(grad * unit, axis=0), jnp.sum(grad, axis=0)


def gelu_parts(values):
    size = jnp.abs(values)
    step = 1.0 / (1.0 + (0.3275911 * 0.7071067811865476) * size)
    bell = jnp.exp(-0.5 * values * values)
    series = step * (
        0.5 * 0.254829592
        + step
        * (
            0.5 * -0.284496736
            + step * (0.5 * 1.421413741 + step * (0.5 * -1.453152027 + step * (0.5 * 1.061405429)))
        )
    )
    low = series * bell
    phi = jnp.where(values < 0.0, low, 1.0 - low)
    return values * phi, phi + values * (bell * 0.3989422804014327)


class Layout:
    def __init__(self, samples, rows_dev):
        self.samples = samples
        self.rows_dev = rows_dev
        self.n_dp = lax.axis_size("dp")
        self.n_wide = lax.axis_size("wide")
        self.parts = self.n_wide // samples
        self.pair = self.parts == 2 and self.n_dp % 2 == 0
        dp, wide = lax.axis_index("dp"), lax.axis_index("wide")
        self.turn = wide // self.parts
        self.part = dp % 2 if self.pair else wide % self.parts

    def shift(self, pieces, step):
        if step == 0 and not self.pair:
            return pieces
        routes = []
        for dp in range(self.n_dp):
            for wide in range(self.n_wide):
                turn, part = divmod(wide, self.parts)
                goal = (turn + step) % self.samples
                if self.pair:
                    target = (dp // 2 * 2 + part) * self.n_wide + goal * 2 + dp % 2
                else:
                    target = dp * self.n_wide + goal * self.parts + part
                source = dp * self.n_wide + wide
                if source != target:
                    routes.append((source, target))
        return lax.ppermute(pieces, AXES, routes)

    def join(self, arrived, own):
        if self.pair:
            stays = lax.axis_index("dp") % 2 == lax.axis_index("wide") % self.parts
            arrived = [jnp.where(stays, own, arrived[0]), *arrived[1:]]
        whole = jnp.zeros((len(arrived),) + own.shape, own.dtype)
        for place, piece in enumerate(arrived):
            whole = whole.at[place].set(piece)
        return whole

    def rows_of(self, part):
        steps = jnp.arange(self.samples, dtype=jnp.int32)
        blocks = (self.turn - steps) % self.samples * self.parts + part
        inside = jnp.arange(self.rows_dev, dtype=jnp.int32)
        return (blocks[:, None] * self.rows_dev + inside[None, :]).reshape(-1)

    def orders(self, freqs):
        if self.pair:
            row_ids = jnp.concatenate([self.rows_of(self.part), self.rows_of(1 - self.part)])
            span = jnp.arange(freqs // 2, dtype=jnp.int32)
            freq_ids = jnp.concatenate(
                [self.part * (freqs // 2) + span, (1 - self.part) * (freqs // 2) + span]
            )
        else:
            row_ids = jnp.concatenate([self.rows_of(part) for part in range(self.parts)])
            freq_ids = jnp.arange(freqs, dtype=jnp.int32)
        return row_ids, freq_ids

    def swap(self, values):
        routes = []
        for dp in range(self.n_dp):
            for wide in range(self.n_wide):
                routes.append((dp * self.n_wide + wide, (dp ^ 1) * self.n_wide + wide))
        return lax.ppermute(values, AXES, routes)

    def groups(self):
        return [
            [turn * self.parts + part for part in range(self.parts)] for turn in range(self.samples)
        ]

    def to_freqs(self, rows):
        if self.pair:
            half = rows.shape[2] // 2
            arrived = self.swap(rows[:, :, half:])
            return jnp.concatenate([rows[:, :, :half], arrived], axis=0)
        return lax.all_to_all(
            rows, "wide", split_axis=2, concat_axis=0, axis_index_groups=self.groups(), tiled=True
        )

    def to_rows(self, cols):
        if self.pair:
            half = cols.shape[0] // 2
            arrived = self.swap(cols[half:])
            return jnp.concatenate([cols[:half], arrived], axis=2)
        return lax.all_to_all(
            cols, "wide", split_axis=0, concat_axis=2, axis_index_groups=self.groups(), tiled=True
        )


def make_tables(grid_height, grid_width, row_ids, freq_ids):
    across = jnp.arange(grid_width, dtype=jnp.int32)
    angles = (
        2.0 * jnp.pi / grid_width * (across[:, None] * freq_ids[None, :] % grid_width).astype(F32)
    )
    row_table = (
        jnp.stack([jnp.cos(angles), -jnp.sin(angles)], axis=1) / jnp.sqrt(F32(grid_width))
    ).astype(BF16)
    doubling = jnp.where(freq_ids == 0, 1.0, 2.0).astype(F32)
    inv_table = (row_table.astype(F32) * doubling).astype(BF16)
    down = jnp.arange(grid_height, dtype=jnp.int32)
    col_angles = (
        2.0 * jnp.pi / grid_height * (down[:, None] * row_ids[None, :] % grid_height).astype(F32)
    )
    cosine = jnp.cos(col_angles) / jnp.sqrt(F32(grid_height))
    sine = jnp.sin(col_angles) / jnp.sqrt(F32(grid_height))
    col_table = jnp.stack([jnp.stack([cosine, sine]), jnp.stack([-sine, cosine])]).astype(BF16)
    return row_table, inv_table, col_table


def bits_of(size):
    count = size.bit_length() - 1
    assert 1 << count == size
    return count


def route_bit(bit, total):
    return [(index, index ^ (1 << bit)) for index in range(total)]


def my_bit(bit):
    index = lax.axis_index("dp") * lax.axis_size("wide") + lax.axis_index("wide")
    return (index >> bit) & 1


def bit_orders():
    wide_bits = bits_of(lax.axis_size("wide"))
    dp_bits = bits_of(lax.axis_size("dp"))
    slow = list(range(wide_bits - 1, 0, -1))
    high = list(range(wide_bits + dp_bits - 1, wide_bits, -1))
    return slow + high + [0, wide_bits], slow + [0] + high + [wide_bits]


def gather_shards(shard, order):
    total = lax.axis_size("dp") * lax.axis_size("wide")
    held, have = shard, []
    for bit in order:
        arrived = lax.ppermute(held, AXES, route_bit(bit, total))
        place = sum(1 for other in have if other > bit)
        mine = my_bit(bit) == 1
        low, high = jnp.where(mine, arrived, held), jnp.where(mine, held, arrived)
        held = jnp.stack([low, high], axis=place)
        have.append(bit)
    return held.reshape((total * shard.shape[0],) + shard.shape[1:])


class Halving:
    def __init__(self, values, order):
        self.total = lax.axis_size("dp") * lax.axis_size("wide")
        count = bits_of(self.total)
        self.left = list(range(count - 1, -1, -1))
        self.order = list(order)
        self.held = values.reshape((2,) * count + (values.shape[0] // self.total, values.shape[1]))
        self.send()

    def send(self):
        bit = self.order.pop(0)
        place = self.left.index(bit)
        mine = my_bit(bit)
        sent = lax.dynamic_index_in_dim(self.held, 1 - mine, place, keepdims=False).astype(BF16)
        self.kept = lax.dynamic_index_in_dim(self.held, mine, place, keepdims=False)
        self.arrived = lax.ppermute(sent, AXES, route_bit(bit, self.total))
        self.left.remove(bit)

    def step(self):
        self.held = self.kept.astype(F32) + self.arrived.astype(F32)
        if self.order:
            self.held = self.held.astype(BF16)
            self.send()

    def finish(self):
        while self.order:
            self.step()
        self.step()
        return self.held


def advance(running, anchor):
    if not running[0].order:
        return anchor
    arrived, anchor = lax.optimization_barrier((tuple(one.arrived for one in running), anchor))
    for one, value in zip(running, arrived):
        one.arrived = value
        one.step()
    return anchor


def sum_kernel(n_dp, n_wide, mine_ref, out_ref, box, own_sem, send_sem, recv_sem):
    total = n_dp * n_wide
    me = lax.axis_index("dp") * n_wide + lax.axis_index("wide")

    def place(index):
        return (index // n_wide, index % n_wide)

    def push(offset):
        return pltpu.make_async_remote_copy(
            src_ref=mine_ref,
            dst_ref=box.at[me],
            send_sem=send_sem.at[offset],
            recv_sem=recv_sem.at[me],
            device_id=place((me + offset) % total),
            device_id_type=pl.DeviceIdType.MESH,
        )

    def pull(offset):
        source = (me + total - offset) % total
        return pltpu.make_async_remote_copy(
            src_ref=mine_ref,
            dst_ref=box.at[source],
            send_sem=send_sem.at[offset],
            recv_sem=recv_sem.at[source],
            device_id=place(source),
            device_id_type=pl.DeviceIdType.MESH,
        )

    barrier = pltpu.get_barrier_semaphore()

    @pl.loop(1, total)
    def _(offset):
        pl.semaphore_signal(
            barrier, inc=1, device_id=place((me + offset) % total), device_id_type=pl.DeviceIdType.MESH
        )

    own = pltpu.make_async_copy(mine_ref, box.at[me], own_sem)
    own.start()
    pl.semaphore_wait(barrier, total - 1)

    @pl.loop(1, total)
    def _(offset):
        push(offset).start()

    own.wait()

    @pl.loop(1, total)
    def _(offset):
        push(offset).wait_send()
        pull(offset).wait_recv()

    out_ref[...] = jnp.sum(box[...], axis=0)


def sum_everywhere(values):
    n_dp, n_wide = lax.axis_size("dp"), lax.axis_size("wide")
    total = n_dp * n_wide

    def kernel(*refs):
        sum_kernel(n_dp, n_wide, *refs)

    return pl.pallas_call(
        kernel,
        out_shape=jax.ShapeDtypeStruct(values.shape, F32),
        in_specs=[pl.BlockSpec(memory_space=pltpu.VMEM)],
        out_specs=pl.BlockSpec(memory_space=pltpu.VMEM),
        scratch_shapes=[
            pltpu.VMEM((total,) + values.shape, F32),
            pltpu.SemaphoreType.DMA,
            pltpu.SemaphoreType.DMA((total,)),
            pltpu.SemaphoreType.DMA((total,)),
        ],
        compiler_params=pltpu.CompilerParams(collective_id=3, has_side_effects=True),
        name="sum_everywhere",
    )(values)


def block_diagonal(weight):
    width, size = weight.shape
    block = jnp.arange(width, dtype=jnp.int32) // size
    return jnp.where(
        block[:, None] == block[None, :], jnp.tile(weight, (1, width // size)), jnp.zeros((), weight.dtype)
    )


def diagonal_blocks(cross, size):
    width = cross.shape[0]
    block = jnp.arange(width, dtype=jnp.int32) // size
    kept = jnp.where(block[:, None] == block[None, :], cross, 0.0)
    return sum(kept[:, start : start + size] for start in range(0, width, size))


def mix(spec, weight, bias):
    last = ((1,), (0,))
    real = dot(spec[0], weight[0], last) - dot(spec[1], weight[1], last) + bias[0]
    imag = dot(spec[0], weight[1], last) + dot(spec[1], weight[0], last) + bias[1]
    return real, imag


def mix_back(d_re, d_im, weight):
    last = ((1,), (1,))
    real = dot(d_re, weight[0], last) + dot(d_im, weight[1], last)
    imag = dot(d_im, weight[0], last) - dot(d_re, weight[1], last)
    return real, imag


def mix_weight(in_re, in_im, d_re, d_im, size):
    first = ((0,), (0,))
    real = dot(in_re, d_re, first) + dot(in_im, d_im, first)
    imag = dot(in_re, d_im, first) - dot(in_im, d_re, first)
    bias = jnp.stack([jnp.sum(d_re, axis=0, dtype=F32), jnp.sum(d_im, axis=0, dtype=F32)])
    return jnp.stack([diagonal_blocks(real, size), diagonal_blocks(imag, size)]), bias


def adam_update(master, moment, square, grad, factor, rate, decay):
    clipped = grad * factor
    moment_next = BETA_ONE * moment + (1.0 - BETA_ONE) * clipped
    square_next = BETA_TWO * square + (1.0 - BETA_TWO) * clipped * clipped
    ratio = (
        moment_next / (1.0 - BETA_ONE**10) / (jnp.sqrt(square_next / (1.0 - BETA_TWO**10)) + 1e-08)
    )
    return (master - rate * (ratio + decay * master), moment_next, square_next)


def train_step(
    fields,
    targets,
    patch_mask,
    channel_mask,
    *state,
):
    masters, moments, squares = state[:6], state[6:12], state[12:]
    samples, rows_dev, grid_width, patch_dim = fields.shape
    layout = Layout(samples, rows_dev)
    grid_height = rows_dev * layout.n_wide
    channels = channel_mask.shape[1]
    pixels = patch_dim // channels
    rows = samples * rows_dev
    tokens = rows * grid_width
    freqs = grid_width // 2
    width_model = masters[0].shape[1]
    size = masters[4].shape[3]

    fields_sent, targets_sent = [], []
    for step in range(samples):
        sample = (layout.turn + step) % samples
        piece = lax.dynamic_index_in_dim(fields, sample, 0, keepdims=False)
        mask = lax.dynamic_index_in_dim(patch_mask, sample, 0, keepdims=False)
        fields_sent.append(piece * mask[..., None].astype(BF16))
        piece = lax.dynamic_index_in_dim(targets, sample, 0, keepdims=False)
        seen = lax.dynamic_index_in_dim(channel_mask, sample, 0, keepdims=False)
        seen = jnp.repeat(seen, pixels)
        used = (mask[..., None] * seen) > 0
        targets_sent.append(jnp.where(used, piece, jnp.asarray(UNUSED, BF16)))
    pieces = [None] * samples
    for step in (*range(1, samples), 0):
        pieces[step] = layout.shift(fields_sent[step], step)

    valid_patch = patch_mask.astype(F32)
    channel_on = channel_mask.astype(F32)
    local_counts = jnp.sum(channel_on * jnp.sum(valid_patch, axis=(1, 2))[:, None], axis=0)
    upper = jnp.floor(local_counts / 256.0)
    digits = jnp.stack([upper, local_counts - 256.0 * upper])

    order_one, order_two = bit_orders()
    shard_rows = masters[4].shape[2]
    mixed = jnp.concatenate(
        [
            masters[4].transpose(2, 0, 1, 3).reshape(shard_rows, 4 * size),
            masters[5].T,
            jnp.pad(digits, ((0, shard_rows - 2), (0, 0))),
        ],
        axis=1,
    ).astype(BF16)
    mixed = jnp.pad(mixed, ((0, 0), (0, -mixed.shape[1] % 128)))
    embed_used = gather_shards(masters[0].astype(BF16), order_two)
    mixed_used = gather_shards(mixed, order_two)
    expand_used = gather_shards(masters[2].astype(BF16), order_two)
    project_used = gather_shards(masters[3].astype(BF16), order_two)
    head_used = gather_shards(masters[1].astype(BF16), order_two)
    gathered = (embed_used, mixed_used, expand_used, project_used, head_used)
    pieces, gathered = lax.optimization_barrier((tuple(pieces), gathered))
    embed_used, mixed_used, expand_used, project_used, head_used = gathered
    inputs = layout.join(pieces, fields_sent[0]).reshape(tokens, patch_dim)
    digits = mixed_used[:, 4 * size + 14 : 4 * size + 14 + channels].astype(F32)
    digits = jnp.sum(digits.reshape(-1, shard_rows, channels), axis=0)
    counts = (256.0 * digits[0] + digits[1]) * pixels
    scale_cols = jnp.repeat(1.0 / (channels * counts), pixels)
    small_used = mixed_used[:, 4 * size : 4 * size + 14].T.astype(F32)
    spectral_used = [
        [
            block_diagonal(mixed_used[:, (2 * layer + side) * size : (2 * layer + side + 1) * size])
            for side in range(2)
        ]
        for layer in range(2)
    ]

    goals = [layout.shift(piece, step) for step, piece in enumerate(targets_sent)]

    row_ids, freq_ids = layout.orders(freqs)
    row_table, inv_table, col_table = make_tables(grid_height, grid_width, row_ids, freq_ids)

    hidden_zero = dot(inputs, embed_used, ((1,), (0,))) + small_used[4]
    unit_one, rstd_one = normalize(hidden_zero)
    normed_one = unit_one * small_used[0] + small_used[1]
    normed_low = normed_one.astype(BF16).reshape(rows, grid_width, width_model)
    rows_freq = jnp.einsum(
        "rwd,wak->rakd", normed_low, row_table, preferred_element_type=F32
    ).astype(BF16)
    rows_moved = layout.to_freqs(rows_freq)
    own_freqs = rows_moved.shape[2]
    spectrum = jnp.einsum(
        "oaxi,iakd->oxkd", col_table, rows_moved, preferred_element_type=F32
    ).astype(BF16)
    spectrum = spectrum.reshape(2, grid_height * own_freqs, width_model)
    first_pre = mix(spectrum, spectral_used[0], small_used[10:12])
    first_act = [jax.nn.relu(part).astype(BF16) for part in first_pre]
    second_pre = mix(first_act, spectral_used[1], small_used[12:14])
    shrunk = jnp.stack(
        [(part - jnp.clip(part, -SHRINK, SHRINK)).astype(BF16) for part in second_pre]
    ).reshape(2, grid_height, own_freqs, width_model)
    open_gate = [jnp.abs(part) > SHRINK for part in second_pre]
    back_cols = jnp.einsum(
        "aoxi,axkd->iokd", col_table, shrunk, preferred_element_type=F32
    ).astype(BF16)
    cols_moved = layout.to_rows(back_cols)
    filtered = jnp.einsum(
        "wak,rakd->rwd", inv_table, cols_moved, preferred_element_type=F32
    ).reshape(tokens, width_model)
    hidden_one = hidden_zero + filtered + normed_one
    unit_two, rstd_two = normalize(hidden_one)
    normed_two = (unit_two * small_used[2] + small_used[3]).astype(BF16)
    expand_pre = dot(normed_two, expand_used, ((1,), (0,))) + small_used[6:10].reshape(-1)
    expand_act, gelu_slope = gelu_parts(expand_pre)
    expand_act, gelu_slope = lax.optimization_barrier(
        (expand_act.astype(BF16), gelu_slope.astype(BF16))
    )
    hidden_two = hidden_one + dot(expand_act, project_used, ((1,), (0,))) + small_used[5]
    hidden_low, goals = lax.optimization_barrier((hidden_two.astype(BF16), tuple(goals)))
    goals = layout.join(goals, targets_sent[0]).reshape(tokens, patch_dim)
    predict = dot(hidden_low, head_used, ((1,), (0,)))

    goals = goals.astype(F32)
    errors = jnp.where(goals < 0.5 * UNUSED, predict - goals, 0.0)
    column_errors = jnp.sum(errors * errors, axis=0)
    grad_low = (2.0 * errors * scale_cols).astype(BF16)

    order_sum_one, order_sum_two = order_one[::-1], order_two[::-1]
    grad_head = dot(hidden_low, grad_low, ((0,), (0,))).astype(BF16)
    sum_head = Halving(grad_head, order_sum_two)
    grad_two = dot(grad_low, head_used, ((1,), (1,)))
    grad_branch = grad_two.astype(BF16)
    grad_project = dot(expand_act, grad_branch, ((0,), (0,))).astype(BF16)
    sum_project = Halving(grad_project, order_sum_two)
    bias_project = jnp.sum(grad_branch, axis=0, dtype=F32)
    grad_act = dot(grad_branch, project_used, ((1,), (1,)))
    grad_pre = (grad_act * gelu_slope).astype(BF16)
    grad_expand = dot(normed_two, grad_pre, ((0,), (0,))).astype(BF16)
    sum_expand = Halving(grad_expand, order_sum_one)
    early = [sum_head, sum_project, sum_expand]
    bias_expand = jnp.sum(grad_pre, axis=0, dtype=F32)
    grad_normed = dot(grad_pre, expand_used, ((1,), (1,)))
    back_one, gain_two, shift_two = norm_back(grad_normed, unit_two, rstd_two, small_used[2])
    grad_one = grad_two + back_one
    grad_filter = grad_one.astype(BF16).reshape(rows, grid_width, width_model)
    grad_cols = jnp.einsum(
        "wak,rwd->rakd", inv_table, grad_filter, preferred_element_type=F32
    ).astype(BF16)
    grad_cols = advance(early, grad_cols)
    grad_moved = layout.to_freqs(grad_cols)
    grad_shrunk = jnp.einsum(
        "aoxi,iokd->axkd", col_table, grad_moved, preferred_element_type=F32
    ).reshape(2, grid_height * own_freqs, width_model)
    d_second = [
        jnp.where(open_gate[side], grad_shrunk[side], 0.0).astype(BF16) for side in range(2)
    ]
    d_second = advance(early, tuple(d_second))
    grad_first_act = mix_back(*d_second, spectral_used[1])
    weight_two, bias_two = mix_weight(*first_act, *d_second, size)
    d_first = [
        jnp.where(first_pre[side] > 0.0, grad_first_act[side], 0.0).astype(BF16)
        for side in range(2)
    ]
    d_first = advance(early, tuple(d_first))
    grad_spectrum = mix_back(*d_first, spectral_used[0])
    weight_one, bias_one = mix_weight(spectrum[0], spectrum[1], *d_first, size)
    grad_spectrum = jnp.stack([part.astype(BF16) for part in grad_spectrum]).reshape(
        2, grid_height, own_freqs, width_model
    )
    grad_rows = jnp.einsum(
        "oaxi,oxkd->iakd", col_table, grad_spectrum, preferred_element_type=F32
    ).astype(BF16)
    grad_rows = advance(early, grad_rows)
    grad_back = layout.to_rows(grad_rows)
    grad_normed_one = (
        jnp.einsum("wak,rakd->rwd", row_table, grad_back, preferred_element_type=F32).reshape(
            tokens, width_model
        )
        + grad_one
    )
    back_zero, gain_one, shift_one = norm_back(grad_normed_one, unit_one, rstd_one, small_used[0])
    grad_zero = (grad_one + back_zero).astype(BF16)
    grad_embed = dot(inputs, grad_zero, ((0,), (0,))).astype(BF16)
    reduced_embed = Halving(grad_embed, order_sum_one).finish()
    reduced_head, reduced_project, reduced_expand = [one.finish() for one in early]
    bias_embed = jnp.sum(grad_zero, axis=0, dtype=F32)
    grad_small = jnp.concatenate(
        [
            jnp.stack([gain_one, shift_one, gain_two, shift_two, bias_embed, bias_project]),
            bias_expand.reshape(4, width_model),
            bias_one,
            bias_two,
        ],
        axis=0,
    )
    grad_mixed = jnp.concatenate(
        [weight_one[0], weight_one[1], weight_two[0], weight_two[1], grad_small.T], axis=1
    )
    grad_mixed = jnp.pad(grad_mixed, ((0, 0), (0, -grad_mixed.shape[1] % 128)))
    reduced_mixed = Halving(grad_mixed, order_sum_two).finish()
    reduced_spectral = (
        reduced_mixed[:, : 4 * size].reshape(shard_rows, 2, 2, size).transpose(1, 2, 0, 3)
    )
    reduced_small = reduced_mixed[:, 4 * size : 4 * size + 14].T
    reduced = (
        reduced_embed,
        reduced_head,
        reduced_expand,
        reduced_project,
        reduced_spectral,
        reduced_small,
    )

    local_square = sum(jnp.sum(grad * grad) for grad in reduced)
    local_error = jnp.sum(column_errors.reshape(channels, pixels), axis=1)
    local_sums = jnp.concatenate([local_error, local_square[None]])
    sums = sum_everywhere(jnp.zeros((8, 128), F32).at[0, : channels + 1].set(local_sums))
    error_sums, total_square = sums[0, :channels], sums[0, channels]
    grad_norm = jnp.sqrt(total_square)
    loss = jnp.sum(error_sums / counts) / channels
    batch = samples * layout.n_dp
    clip_level = 0.25 / jnp.sqrt(F32(batch * grid_height * grid_width))
    factor = jnp.minimum(1.0, clip_level / grad_norm)
    results = [loss, grad_norm]
    for index in range(6):
        results.extend(
            adam_update(
                masters[index],
                moments[index],
                squares[index],
                reduced[index],
                factor,
                RATES[index],
                DECAYS[index],
            )
        )
    return tuple(results)


def solution(mesh):
    placed = (
        P("dp", "wide", None, None),
        P("dp", "wide", None, None),
        P("dp", "wide", None),
        P("dp", None),
        P(("dp", "wide"), None),
        P(("dp", "wide"), None),
        P(("dp", "wide"), None),
        P(("dp", "wide"), None),
        P(None, None, ("dp", "wide"), None),
        P(None, ("dp", "wide")),
        P(("dp", "wide"), None),
        P(("dp", "wide"), None),
        P(("dp", "wide"), None),
        P(("dp", "wide"), None),
        P(None, None, ("dp", "wide"), None),
        P(None, ("dp", "wide")),
        P(("dp", "wide"), None),
        P(("dp", "wide"), None),
        P(("dp", "wide"), None),
        P(("dp", "wide"), None),
        P(None, None, ("dp", "wide"), None),
        P(None, ("dp", "wide")),
    )
    return jax.shard_map(
        train_step,
        mesh=mesh,
        in_specs=placed,
        out_specs=(
            P(),
            P(),
            P(("dp", "wide"), None),
            P(("dp", "wide"), None),
            P(("dp", "wide"), None),
            P(("dp", "wide"), None),
            P(("dp", "wide"), None),
            P(("dp", "wide"), None),
            P(("dp", "wide"), None),
            P(("dp", "wide"), None),
            P(("dp", "wide"), None),
            P(("dp", "wide"), None),
            P(("dp", "wide"), None),
            P(("dp", "wide"), None),
            P(None, None, ("dp", "wide"), None),
            P(None, None, ("dp", "wide"), None),
            P(None, None, ("dp", "wide"), None),
            P(None, ("dp", "wide")),
            P(None, ("dp", "wide")),
            P(None, ("dp", "wide")),
        ),
        check_vma=False,
    )
```
